32 devices in a mesh: aux: 8 (over z, x), row: 4 (over y, core).
Axes of the slice: x: 2, y: 2, z: 4, core: 2. Of those that a mesh axis runs over, the one named last changes fastest.
Arguments:
- slabs: bfloat16 [64, 400, 2048], P('aux', None, 'row'), may hold values from -0.47265625 to 0.47265625
- significant: int32 [64, 32], P('aux'), may hold values from 0 to 1, as said below
Outputs:
- exchange: float32 [2048, 2048], P('row', 'aux')
The draws below stay inside these ranges and needn't reach their ends.
Inputs may be any that keep to these rules, and one draw needn't show every extreme that they name: `significant`: each entry is 0 or 1; the share of ones differs between the auxiliary functions of different devices.
All inputs are finite; a program needn't handle non-finite values.
Results may differ from the reference program's by a relative error of at most 0.0003.
Values may be sent and summed in bfloat16 or wider, within the bound.
A program may use at most 64 MiB of HBM per device.

```python
import jax
import jax.numpy as jnp
from jax import lax

NBF = 2048
NOCC = 400
BS = 64
AUX_DEV = 8
NAUXW = 64
NBLK = 32


def draw_significant(key, part):
    first_key, second_key = jax.random.split(jax.random.fold_in(key, 11))
    groups = NAUXW // AUX_DEV
    levels = jax.random.randint(first_key, (groups, 1, 1), 3, 19)
    levels = jnp.broadcast_to(levels, (groups, AUX_DEV, NBLK)).reshape(NAUXW, NBLK)
    rolled = jax.random.randint(second_key, (NAUXW, NBLK), 0, 20)
    return (rolled < levels).astype(jnp.int32)


def block_levels(own_key, extent, cuts, low, largest):
    def one(position, blocks):
        draws = jax.random.uniform(jax.random.fold_in(jax.random.fold_in(own_key, 6), position), (blocks,), jnp.float32, low / len(cuts), largest / len(cuts))
        return jnp.repeat(jnp.exp(draws), extent[position] // blocks).reshape((-1,) + (1,) * (len(extent) - position - 1))

    level = one(*cuts[0])
    for cut in cuts[1:]:
        level = level * one(*cut)
    return level


def scatter_about(rng, extent, scale, most, cuts=(), held_as=jnp.bfloat16):
    level = block_levels(rng, extent, cuts, -0.22, 0.18) if cuts else 1.0
    entries = jax.random.normal(rng, extent, jnp.float32) * scale * level
    return jnp.minimum(jnp.maximum(entries, -most), most).astype(held_as)


def setup_inputs(seed: int = 0) -> dict:
    key_of = jax.random.split(jax.random.key(seed), 3)
    return {
        "slabs": scatter_about(key_of[0], (NAUXW, NOCC, NBF), ((NAUXW * NOCC) ** -0.25), 0.47265625, ((0, 8), (2, 4))),
        "significant": draw_significant(jax.random.fold_in(key_of[2], 71), 0),
    }


def reference(slabs, significant):
    block_of = lax.broadcasted_iota(jnp.int32, (NBLK, NBF), 1) // BS
    block_id = lax.broadcasted_iota(jnp.int32, (NBLK, NBF), 0)
    expand_table = (block_of == block_id).astype(jnp.float32)
    column_mask = jnp.dot(significant.astype(jnp.float32), expand_table).astype(jnp.bfloat16)
    masked = (slabs * column_mask[:, None, :]).reshape(NAUXW * NOCC, NBF)
    return lax.dot_general(masked, masked, (((0,), (0,)), ((), ())), preferred_element_type=jnp.float32)
```

```python
import functools

import jax
import jax.numpy as jnp
from jax import lax
from jax.experimental import pallas as pl
from jax.experimental.pallas import tpu as pltpu
from jax.sharding import PartitionSpec as P

BS = 64
LANES = 128
SUB = 128
LAG = 3


def plain(slabs, significant):
    aux_here, occupied, rows_here = slabs.shape
    blocks_here = rows_here // BS
    first_block = lax.axis_index("row") * blocks_here
    local_mask = lax.dynamic_slice_in_dim(significant, first_block, blocks_here, 1).astype(
        jnp.float32
    )
    block_of = lax.broadcasted_iota(jnp.int32, (blocks_here, rows_here), 1) // BS
    block_id = lax.broadcasted_iota(jnp.int32, (blocks_here, rows_here), 0)
    expand_table = (block_of == block_id).astype(jnp.float32)
    column_mask = jnp.dot(local_mask, expand_table).astype(jnp.bfloat16)
    masked = (slabs * column_mask[:, None, :]).reshape(aux_here * occupied, rows_here)
    partial_rows = lax.dot_general(
        masked,
        lax.all_gather(masked, "row", axis=1, tiled=True),
        (((0,), (0,)), ((), ())),
        preferred_element_type=jnp.float32,
    )
    return lax.psum_scatter(partial_rows, "aux", scatter_dimension=1, tiled=True)


def kernel(n_aux, n_row, occupied, slab_hbm, mask_ref, out_ref, g, lhs_t, mk, ps, xr, zb, zlo, zhi,
           own_sem, psend, precv, ysend, yrecv, fsend, frecv, xsend, xrecv, zsend, zlo_sem, zhi_sem):
    depth = slab_hbm.shape[0]
    chunks = g.shape[1]
    rows = ps.shape[3]
    subs = rows // SUB
    width = chunks * LANES
    a, r = lax.axis_index("aux"), lax.axis_index("row")
    z, x = a // 2, a % 2
    last = n_aux // 2 - 1
    y, c = r // 2, r % 2
    partner = y * 2 + (1 - c)
    across = (1 - y) * 2 + c
    owner = (r, partner, across, (1 - y) * 2 + (1 - c))
    beside = z * 2 + (1 - x)

    barrier = pltpu.get_barrier_semaphore()
    for there in ({"row": partner}, {"row": across}, {"aux": beside},
                  {"aux": lax.rem(a + 2, n_aux)}, {"aux": lax.rem(a + n_aux - 2, n_aux)}):
        pl.semaphore_signal(barrier, inc=1, device_id=there, device_id_type=pl.DeviceIdType.MESH)

    def piece(j, h):
        return slab_hbm.at[:, pl.ds(h * width + j * LANES, LANES)]

    def remote(src, dst, send, recv, there):
        return pltpu.make_async_remote_copy(
            src_ref=src, dst_ref=dst, send_sem=send, recv_sem=recv, device_id=there,
            device_id_type=pl.DeviceIdType.MESH,
        )

    both = [(j, h) for j in range(chunks) for h in range(2)]
    own = {w: pltpu.make_async_copy(piece(*w), g.at[(0,) + w], own_sem.at[w]) for w in both}
    for w in both:
        own[w].start()
    pl.semaphore_wait(barrier, 5)
    to_y = {w: remote(piece(*w), g.at[(2,) + w], ysend.at[w], yrecv.at[w], {"row": across}) for w in both}
    to_p = {w: remote(piece(*w), g.at[(1,) + w], psend.at[w], precv.at[w], {"row": partner}) for w in both}
    fwd = {w: remote(g.at[(2,) + w], g.at[(3,) + w], fsend.at[w], frecv.at[w], {"row": partner}) for w in both}
    for w in both:
        to_y[w].start()
    for w in both:
        to_p[w].start()

    def masked(k, j, h):
        raw = g[k, j, h].reshape(-1, occupied // 16, 16, LANES)
        return (raw * mask_ref[owner[k], h, j][:, None]).reshape(depth, LANES)

    def x_copy(k, j, s):
        part = pl.ds(s * SUB, SUB)
        return remote(ps.at[k, j, 1 - x, part], xr.at[k, j, part], xsend.at[k, j, s], xrecv.at[k, j, s],
                      {"aux": beside})

    def z_copy(k, j, s, up):
        part = pl.ds(s * SUB, SUB)
        land, sem = (zlo, zlo_sem) if up else (zhi, zhi_sem)
        return remote(zb.at[k, j, part], land.at[k, j, part], zsend.at[k, j, s], sem.at[k, j, s],
                      {"aux": jnp.minimum(a + 2, n_aux - 1) if up else jnp.maximum(a - 2, 0)})

    def multiply(k, j):
        for h in range(2):
            mk[:, h * LANES:(h + 1) * LANES] = masked(k, j, h)

        @pl.loop(0, subs)
        def _(s):
            part = pl.ds(pl.multiple_of(s * SUB, SUB), SUB)
            acc = jnp.dot(lhs_t[part, :], mk[...], preferred_element_type=jnp.float32)
            ps[k, j, 0, part, :] = acc[:, :LANES]
            ps[k, j, 1, part, :] = acc[:, LANES:]

        for s in range(subs):
            x_copy(k, j, s).start()

    def sum_x(k, j, s):
        d = owner[k]
        part = pl.ds(s * SUB, SUB)
        x_copy(k, j, s).wait_recv()
        zb[k, j, part, :] = ps[k, j, x, part, :] + xr[k, j, part, :]
        pl.when((z == 0) & (d > 0))(lambda: z_copy(k, j, s, True).start())
        pl.when((z == last) & (d < last))(lambda: z_copy(k, j, s, False).start())

    def sum_z(k, j, s):
        d = owner[k]
        part = pl.ds(s * SUB, SUB)

        @pl.when((z > 0) & (z <= d))
        def _():
            z_copy(k, j, s, True).wait_recv()
            zb[k, j, part, :] += zlo[k, j, part, :]

        @pl.when((z < last) & (z >= d))
        def _():
            z_copy(k, j, s, False).wait_recv()
            zb[k, j, part, :] += zhi[k, j, part, :]

        pl.when((z > 0) & (z < d))(lambda: z_copy(k, j, s, True).start())
        pl.when((z < last) & (z > d))(lambda: z_copy(k, j, s, False).start())

        @pl.when(z == d)
        def _():
            out_ref[part, j * LANES:(j + 1) * LANES] = zb[k, j, part, :]

    def reduce(jobs):
        for t in range(len(jobs) + LAG):
            if t < len(jobs):
                sum_x(*jobs[t])
            if t >= LAG:
                sum_z(*jobs[t - LAG])

    for j, h in both:
        own[j, h].wait()
        mk[:, :LANES] = masked(0, j, h)
        lhs_t[h * width + j * LANES:h * width + (j + 1) * LANES, :] = mk[:, :LANES].T
    for j in range(chunks):
        multiply(0, j)
    for j in range(chunks):
        for h in range(2):
            to_p[j, h].wait_recv()
        multiply(1, j)
    reduce([(k, j, s) for k in range(2) for j in range(chunks) for s in range(subs)])
    for j in range(chunks):
        for h in range(2):
            to_y[j, h].wait_recv()
            fwd[j, h].start()
        multiply(2, j)
        for h in range(2):
            fwd[j, h].wait_recv()
        multiply(3, j)
        reduce([(k, j, s) for k in (2, 3) for s in range(subs)])

    for w in both:
        to_y[w].wait_send()
        to_p[w].wait_send()
        fwd[w].wait_send()
    for k in range(n_row):
        for j in range(chunks):
            for s in range(subs):
                x_copy(k, j, s).wait_send()
                pl.when(z != owner[k])(lambda: z_copy(k, j, s, True).wait_send())


def solution(mesh):
    n_aux, n_row = mesh.shape["aux"], mesh.shape["row"]

    def local(slabs, significant):
        aux_here, occupied, rows = slabs.shape
        nbf = rows * n_row
        cols = nbf // n_aux
        if n_row != 4 or n_aux != 2 * n_row or cols % LANES or rows % SUB or occupied % 16:
            return plain(slabs, significant)
        chunks = cols // LANES
        depth = aux_here * occupied
        mask = jnp.repeat(significant.astype(jnp.bfloat16), BS, axis=1)
        mask = mask.reshape(aux_here, n_row, 2, chunks, LANES).transpose(1, 2, 3, 0, 4)
        mask = jnp.broadcast_to(mask[:, :, :, :, None], (n_row, 2, chunks, aux_here, 16, LANES))
        dma = pltpu.SemaphoreType.DMA
        subs = rows // SUB
        return pl.pallas_call(
            functools.partial(kernel, n_aux, n_row, occupied),
            out_shape=jax.ShapeDtypeStruct((rows, cols), jnp.float32),
            in_specs=[pl.BlockSpec(memory_space=pl.ANY), pl.BlockSpec(memory_space=pltpu.VMEM)],
            out_specs=pl.BlockSpec(memory_space=pltpu.VMEM),
            scratch_shapes=[
                pltpu.VMEM((n_row, chunks, 2, depth, LANES), jnp.bfloat16),
                pltpu.VMEM((rows, depth), jnp.bfloat16),
                pltpu.VMEM((depth, 2 * LANES), jnp.bfloat16),
                pltpu.VMEM((n_row, chunks, 2, rows, LANES), jnp.float32),
            ]
            + [pltpu.VMEM((n_row, chunks, rows, LANES), jnp.float32)] * 4
            + [dma((chunks, 2))] * 7
            + [dma((n_row, chunks, subs))] * 5,
            compiler_params=pltpu.CompilerParams(
                collective_id=0, has_side_effects=True, vmem_limit_bytes=60 * 2**20
            ),
            cost_estimate=pl.CostEstimate(
                flops=2 * rows * nbf * depth, bytes_accessed=2 * depth * rows, transcendentals=0
            ),
        )(slabs.reshape(depth, rows), mask)

    return jax.shard_map(
        local,
        mesh=mesh,
        in_specs=(P("aux", None, "row"), P("aux", None)),
        out_specs=P("row", "aux"),
        check_vma=False,
    )
```

```python
import functools

import jax
import jax.numpy as jnp
from jax import lax
from jax.experimental import pallas as pl
from jax.experimental.pallas import tpu as pltpu
from jax.sharding import PartitionSpec as P

BS = 64
LANES = 128
SUB = 128
LAG = 3


def plain(slabs, significant):
    aux_here, occupied, rows_here = slabs.shape
    blocks_here = rows_here // BS
    first_block = lax.axis_index("row") * blocks_here
    local_mask = lax.dynamic_slice_in_dim(significant, first_block, blocks_here, 1).astype(
        jnp.float32
    )
    block_of = lax.broadcasted_iota(jnp.int32, (blocks_here, rows_here), 1) // BS
    block_id = lax.broadcasted_iota(jnp.int32, (blocks_here, rows_here), 0)
    expand_table = (block_of == block_id).astype(jnp.float32)
    column_mask = jnp.dot(local_mask, expand_table).astype(jnp.bfloat16)
    masked = (slabs * column_mask[:, None, :]).reshape(aux_here * occupied, rows_here)
    partial_rows = lax.dot_general(
        masked,
        lax.all_gather(masked, "row", axis=1, tiled=True),
        (((0,), (0,)), ((), ())),
        preferred_element_type=jnp.float32,
    )
    return lax.psum_scatter(partial_rows, "aux", scatter_dimension=1, tiled=True)


def kernel(n_aux, n_row, occupied, slab_hbm, mask_ref, out_ref, g, gy, lhs_t, mk, ps, xr, zb, zlo, zhi, mr,
           own_sem, psend, precv, ysend, yrecv, fsend, frecv, xsend, xrecv, zsend, zlo_sem, zhi_sem, msend, mrecv):
    depth = slab_hbm.shape[0]
    half = depth // 2
    chunks = g.shape[1]
    rows = ps.shape[3]
    subs = rows // SUB
    width = chunks * LANES
    a, r = lax.axis_index("aux"), lax.axis_index("row")
    z, x = a // 2, a % 2
    last = n_aux // 2 - 1
    y, c = r // 2, r % 2
    partner = y * 2 + (1 - c)
    across = (1 - y) * 2 + c
    owner = (r, partner, across, (1 - y) * 2 + (1 - c))
    beside = z * 2 + (1 - x)

    barrier = pltpu.get_barrier_semaphore()
    for there in ({"row": partner}, {"row": across}, {"aux": beside},
                  {"aux": lax.rem(a + 2, n_aux)}, {"aux": lax.rem(a + n_aux - 2, n_aux)}):
        pl.semaphore_signal(barrier, inc=1, device_id=there, device_id_type=pl.DeviceIdType.MESH)

    def piece(j, h):
        return slab_hbm.at[:, pl.ds(h * width + j * LANES, LANES)]

    def half_piece(j, h):
        first = pl.multiple_of((1 - y) * half, 16)
        return slab_hbm.at[pl.ds(first, half), pl.ds(h * width + j * LANES, LANES)]

    def remote(src, dst, send, recv, there):
        return pltpu.make_async_remote_copy(
            src_ref=src, dst_ref=dst, send_sem=send, recv_sem=recv, device_id=there,
            device_id_type=pl.DeviceIdType.MESH,
        )

    both = [(j, h) for j in range(chunks) for h in range(2)]
    own = {w: pltpu.make_async_copy(piece(*w), g.at[(0,) + w], own_sem.at[w]) for w in both}
    for w in both:
        own[w].start()
    mirrored = z // 2 != y
    tiles = 2 * chunks

    @pl.when(mirrored)
    def _():
        for q in range(2):
            pl.semaphore_signal(barrier, inc=1, device_id={"aux": r * 2 + q, "row": z},
                                device_id_type=pl.DeviceIdType.MESH)

    pl.semaphore_wait(barrier, jnp.where(mirrored, 7, 5))
    to_y = {w: remote(half_piece(*w), gy.at[(0,) + w], ysend.at[w], yrecv.at[w], {"row": across}) for w in both}
    to_p = {w: remote(piece(*w), g.at[(1,) + w], psend.at[w], precv.at[w], {"row": partner}) for w in both}
    fwd = {w: remote(gy.at[(0,) + w], gy.at[(1,) + w], fsend.at[w], frecv.at[w], {"row": partner}) for w in both}
    for w in both:
        to_y[w].start()
    for w in both:
        to_p[w].start()

    def masked(k, j, h):
        if k < 2:
            raw, mask = g[k, j, h], mask_ref[owner[k], h, j]
        else:
            here = half // occupied
            raw, mask = gy[k - 2, j, h], mask_ref[owner[k], h, j, pl.ds(y * here, here)]
        return (raw.reshape(-1, occupied // 16, 16, LANES) * mask[:, None]).reshape(raw.shape)

    def x_copy(k, j, s):
        part = pl.ds(s * SUB, SUB)
        return remote(ps.at[k, j, 1 - x, part], xr.at[k, j, part], xsend.at[k, j, s], xrecv.at[k, j, s],
                      {"aux": beside})

    def z_copy(k, j, s, up):
        part = pl.ds(s * SUB, SUB)
        land, sem = (zlo, zlo_sem) if up else (zhi, zhi_sem)
        return remote(zb.at[k, j, part], land.at[k, j, part], zsend.at[k, j, s], sem.at[k, j, s],
                      {"aux": jnp.minimum(a + 2, n_aux - 1) if up else jnp.maximum(a - 2, 0)})

    def multiply(k, j):
        for h in range(2):
            mk[:depth if k < 2 else half, h * LANES:(h + 1) * LANES] = masked(k, j, h)

        @pl.loop(0, subs)
        def _(s):
            part = pl.ds(pl.multiple_of(s * SUB, SUB), SUB)
            if k < 2:
                acc = jnp.dot(lhs_t[0, part, :], mk[:half, :], preferred_element_type=jnp.float32)
                acc += jnp.dot(lhs_t[1, part, :], mk[half:, :], preferred_element_type=jnp.float32)
            else:
                acc = jnp.dot(lhs_t[y, part, :], mk[:half, :], preferred_element_type=jnp.float32)
            ps[k, j, 0, part, :] = acc[:, :LANES]
            ps[k, j, 1, part, :] = acc[:, LANES:]

        for s in range(subs):
            x_copy(k, j, s).start()

    def m_copy(k, j, s):
        to = x * chunks + j
        return remote(zb.at[k, j, pl.ds(s * SUB, SUB)], mr.at[s % chunks, to], msend.at[j, s],
                      mrecv.at[s % chunks, to], {"aux": r * 2 + s // chunks, "row": z})

    def sum_x(k, j, s):
        d = owner[k]
        part = pl.ds(s * SUB, SUB)
        x_copy(k, j, s).wait_recv()
        zb[k, j, part, :] = ps[k, j, x, part, :] + xr[k, j, part, :]
        pl.when((z == 0) & (d > 0))(lambda: z_copy(k, j, s, True).start())
        pl.when((z == last) & (d < last))(lambda: z_copy(k, j, s, False).start())

    def sum_z(k, j, s):
        d = owner[k]
        part = pl.ds(s * SUB, SUB)

        @pl.when((z > 0) & (z <= d))
        def _():
            z_copy(k, j, s, True).wait_recv()
            zb[k, j, part, :] += zlo[k, j, part, :]

        @pl.when((z < last) & (z >= d))
        def _():
            z_copy(k, j, s, False).wait_recv()
            zb[k, j, part, :] += zhi[k, j, part, :]

        pl.when((z > 0) & (z < d))(lambda: z_copy(k, j, s, True).start())
        pl.when((z < last) & (z > d))(lambda: z_copy(k, j, s, False).start())

        @pl.when(z == d)
        def _():
            if k < 2:
                out_ref[part, j * LANES:(j + 1) * LANES] = zb[k, j, part, :]
            else:
                m_copy(k, j, s).start()

    def reduce(jobs):
        for t in range(len(jobs) + LAG):
            if t < len(jobs):
                sum_x(*jobs[t])
            if t >= LAG:
                sum_z(*jobs[t - LAG])

    for j, h in both:
        own[j, h].wait()
        mk[:, :LANES] = masked(0, j, h)
        for e in range(2):
            lhs_t[e, h * width + j * LANES:h * width + (j + 1) * LANES, :] = mk[e * half:(e + 1) * half, :LANES].T
    for j in range(chunks):
        multiply(0, j)
    for j in range(chunks):
        for h in range(2):
            to_p[j, h].wait_recv()
        multiply(1, j)
    reduce([(k, j, s) for k in range(2) for j in range(chunks) for s in range(subs)])
    for j in range(chunks):
        for h in range(2):
            to_y[j, h].wait_recv()
            fwd[j, h].start()
        multiply(2, j)
        for h in range(2):
            fwd[j, h].wait_recv()
        multiply(3, j)
        reduce([(k, j, s) for k in (2, 3) for s in range(subs)])

    @pl.when(mirrored)
    def _():
        mine = jnp.where(z == across, 2, 3)
        for first in range(chunks):
            for s in range(first, tiles, chunks):
                for j in range(chunks):
                    part = pl.ds(s * SUB, SUB)
                    remote(zb.at[mine, j, part], mr.at[j, s], msend.at[j, s], mrecv.at[j, s],
                           {"aux": r * 2, "row": z}).wait_recv()
                    out_ref[part, j * LANES:(j + 1) * LANES] = zb[mine, j, part, :] + mr[j, s].T
        for j in range(chunks):
            for s in range(tiles):
                m_copy(mine, j, s).wait_send()

    for w in both:
        to_y[w].wait_send()
        to_p[w].wait_send()
        fwd[w].wait_send()
    for k in range(n_row):
        for j in range(chunks):
            for s in range(subs):
                x_copy(k, j, s).wait_send()
                pl.when(z != owner[k])(lambda: z_copy(k, j, s, True).wait_send())


def solution(mesh):
    n_aux, n_row = mesh.shape["aux"], mesh.shape["row"]

    def local(slabs, significant):
        aux_here, occupied, rows = slabs.shape
        nbf = rows * n_row
        cols = nbf // n_aux
        if n_row != 4 or n_aux != 2 * n_row or cols % LANES or rows % SUB or occupied % 16 or aux_here % 2:
            return plain(slabs, significant)
        chunks = cols // LANES
        depth = aux_here * occupied
        mask = jnp.repeat(significant.astype(jnp.bfloat16), BS, axis=1)
        mask = mask.reshape(aux_here, n_row, 2, chunks, LANES).transpose(1, 2, 3, 0, 4)
        mask = jnp.broadcast_to(mask[:, :, :, :, None], (n_row, 2, chunks, aux_here, 16, LANES))
        dma = pltpu.SemaphoreType.DMA
        subs = rows // SUB
        return pl.pallas_call(
            functools.partial(kernel, n_aux, n_row, occupied),
            out_shape=jax.ShapeDtypeStruct((rows, cols), jnp.float32),
            in_specs=[pl.BlockSpec(memory_space=pl.ANY), pl.BlockSpec(memory_space=pltpu.VMEM)],
            out_specs=pl.BlockSpec(memory_space=pltpu.VMEM),
            scratch_shapes=[
                pltpu.VMEM((2, chunks, 2, depth, LANES), jnp.bfloat16),
                pltpu.VMEM((2, chunks, 2, depth // 2, LANES), jnp.bfloat16),
                pltpu.VMEM((2, rows, depth // 2), jnp.bfloat16),
                pltpu.VMEM((depth, 2 * LANES), jnp.bfloat16),
                pltpu.VMEM((n_row, chunks, 2, rows, LANES), jnp.float32),
            ]
            + [pltpu.VMEM((n_row, chunks, rows, LANES), jnp.float32)] * 4
            + [pltpu.VMEM((chunks, subs, SUB, LANES), jnp.float32)]
            + [dma((chunks, 2))] * 7
            + [dma((n_row, chunks, subs))] * 5
            + [dma((chunks, subs))] * 2,
            compiler_params=pltpu.CompilerParams(
                collective_id=0, has_side_effects=True, vmem_limit_bytes=60 * 2**20
            ),
            cost_estimate=pl.CostEstimate(
                flops=2 * rows * nbf * depth, bytes_accessed=2 * depth * rows, transcendentals=0
            ),
        )(slabs.reshape(depth, rows), mask)

    return jax.shard_map(
        local,
        mesh=mesh,
        in_specs=(P("aux", None, "row"), P("aux", None)),
        out_specs=P("row", "aux"),
        check_vma=False,
    )
```

```python
import functools

import jax
import jax.numpy as jnp
from jax import lax
from jax.experimental import pallas as pl
from jax.experimental.pallas import tpu as pltpu
from jax.sharding import PartitionSpec as P

BS = 64
LANES = 128
SUB = 128
LAG = 3


def plain(slabs, significant):
    aux_here, occupied, rows_here = slabs.shape
    blocks_here = rows_here // BS
    first_block = lax.axis_index("row") * blocks_here
    local_mask = lax.dynamic_slice_in_dim(significant, first_block, blocks_here, 1).astype(
        jnp.float32
    )
    block_of = lax.broadcasted_iota(jnp.int32, (blocks_here, rows_here), 1) // BS
    block_id = lax.broadcasted_iota(jnp.int32, (blocks_here, rows_here), 0)
    expand_table = (block_of == block_id).astype(jnp.float32)
    column_mask = jnp.dot(local_mask, expand_table).astype(jnp.bfloat16)
    masked = (slabs * column_mask[:, None, :]).reshape(aux_here * occupied, rows_here)
    partial_rows = lax.dot_general(
        masked,
        lax.all_gather(masked, "row", axis=1, tiled=True),
        (((0,), (0,)), ((), ())),
        preferred_element_type=jnp.float32,
    )
    return lax.psum_scatter(partial_rows, "aux", scatter_dimension=1, tiled=True)


def kernel(n_aux, n_row, occupied, slab_hbm, mask_ref, out_ref, g, gy, lhs_t, mk, ps, xr, zb, zlo, zhi, mr,
           own_sem, psend, precv, ysend, yrecv, fsend, frecv, xsend, xrecv, zsend, zlo_sem, zhi_sem, msend, mrecv):
    depth = slab_hbm.shape[0]
    half = depth // 2
    chunks = g.shape[1]
    rows = ps.shape[3]
    subs = rows // SUB
    width = chunks * LANES
    a, r = lax.axis_index("aux"), lax.axis_index("row")
    z, x = a // 2, a % 2
    last = n_aux // 2 - 1
    y, c = r // 2, r % 2
    partner = y * 2 + (1 - c)
    across = (1 - y) * 2 + c
    owner = (r, partner, across, (1 - y) * 2 + (1 - c))
    beside = z * 2 + (1 - x)

    barrier = pltpu.get_barrier_semaphore()
    for there in ({"row": partner}, {"row": across}, {"aux": beside},
                  {"aux": lax.rem(a + 2, n_aux)}, {"aux": lax.rem(a + n_aux - 2, n_aux)}):
        pl.semaphore_signal(barrier, inc=1, device_id=there, device_id_type=pl.DeviceIdType.MESH)

    def piece(j, h):
        return slab_hbm.at[:, pl.ds(h * width + j * LANES, LANES)]

    def half_piece(j, h):
        first = pl.multiple_of((1 - y) * half, 16)
        return slab_hbm.at[pl.ds(first, half), pl.ds(h * width + j * LANES, LANES)]

    def remote(src, dst, send, recv, there):
        return pltpu.make_async_remote_copy(
            src_ref=src, dst_ref=dst, send_sem=send, recv_sem=recv, device_id=there,
            device_id_type=pl.DeviceIdType.MESH,
        )

    both = [(j, h) for j in range(chunks) for h in range(2)]
    own = {w: pltpu.make_async_copy(piece(*w), g.at[(0,) + w], own_sem.at[w]) for w in both}
    for w in both:
        own[w].start()
    mirrored = z // 2 != y
    tiles = 2 * chunks

    @pl.when(mirrored)
    def _():
        for q in range(2):
            pl.semaphore_signal(barrier, inc=1, device_id={"aux": r * 2 + q, "row": z},
                                device_id_type=pl.DeviceIdType.MESH)

    pl.semaphore_wait(barrier, jnp.where(mirrored, 7, 5))
    to_y = {w: remote(half_piece(*w), gy.at[(0,) + w], ysend.at[w], yrecv.at[w], {"row": across}) for w in both}
    to_p = {w: remote(piece(*w), g.at[(1,) + w], psend.at[w], precv.at[w], {"row": partner}) for w in both}
    fwd = {w: remote(gy.at[(0,) + w], gy.at[(1,) + w], fsend.at[w], frecv.at[w], {"row": partner}) for w in both}
    for w in both:
        to_y[w].start()
    for w in both:
        to_p[w].start()

    def masked(k, j, h):
        if k < 2:
            raw, mask = g[k, j, h], mask_ref[owner[k], h, j]
        else:
            here = half // occupied
            raw, mask = gy[k - 2, j, h], mask_ref[owner[k], h, j, pl.ds(y * here, here)]
        return (raw.reshape(-1, occupied // 16, 16, LANES) * mask[:, None]).reshape(raw.shape)

    def x_copy(k, j, s):
        part = pl.ds(s * SUB, SUB)
        return remote(ps.at[k, j, 1 - x, part], xr.at[k, j, part], xsend.at[k, j, s], xrecv.at[k, j, s],
                      {"aux": beside})

    def z_copy(k, j, s, up):
        part = pl.ds(s * SUB, SUB)
        land, sem = (zlo, zlo_sem) if up else (zhi, zhi_sem)
        return remote(zb.at[k, j, part], land.at[k, j, part], zsend.at[k, j, s], sem.at[k, j, s],
                      {"aux": jnp.minimum(a + 2, n_aux - 1) if up else jnp.maximum(a - 2, 0)})

    def multiply(k, j):
        for h in range(2):
            mk[:depth if k < 2 else half, h * LANES:(h + 1) * LANES] = masked(k, j, h)

        @pl.loop(0, subs)
        def _(s):
            part = pl.ds(pl.multiple_of(s * SUB, SUB), SUB)
            if k < 2:
                acc = jnp.dot(lhs_t[0, part, :], mk[:half, :], preferred_element_type=jnp.float32)
                acc += jnp.dot(lhs_t[1, part, :], mk[half:, :], preferred_element_type=jnp.float32)
            else:
                acc = jnp.dot(lhs_t[y, part, :], mk[:half, :], preferred_element_type=jnp.float32)
            ps[k, j, 0, part, :] = acc[:, :LANES]
            ps[k, j, 1, part, :] = acc[:, LANES:]

        for s in range(subs):
            x_copy(k, j, s).start()

    def m_copy(k, j, s):
        to = x * chunks + j
        return remote(zb.at[k, j, pl.ds(s * SUB, SUB)], mr.at[s % chunks, to], msend.at[j, s],
                      mrecv.at[s % chunks, to], {"aux": r * 2 + s // chunks, "row": z})

    def sum_x(k, j, s):
        d = owner[k]
        part = pl.ds(s * SUB, SUB)
        x_copy(k, j, s).wait_recv()
        zb[k, j, part, :] = ps[k, j, x, part, :] + xr[k, j, part, :]
        pl.when((z == 0) & (d > 0))(lambda: z_copy(k, j, s, True).start())
        pl.when((z == last) & (d < last))(lambda: z_copy(k, j, s, False).start())

    def sum_z(k, j, s):
        d = owner[k]
        part = pl.ds(s * SUB, SUB)

        @pl.when((z > 0) & (z <= d))
        def _():
            z_copy(k, j, s, True).wait_recv()
            zb[k, j, part, :] += zlo[k, j, part, :]

        @pl.when((z < last) & (z >= d))
        def _():
            z_copy(k, j, s, False).wait_recv()
            zb[k, j, part, :] += zhi[k, j, part, :]

        pl.when((z > 0) & (z < d))(lambda: z_copy(k, j, s, True).start())
        pl.when((z < last) & (z > d))(lambda: z_copy(k, j, s, False).start())

        @pl.when(z == d)
        def _():
            if k < 2:
                out_ref[part, j * LANES:(j + 1) * LANES] = zb[k, j, part, :]
            else:
                m_copy(k, j, s).start()

    jobs = []
    hops = [jnp.where(z < d, z, jnp.where(z > d, last - z, jnp.maximum(d, last - d))) for d in owner]

    def sum_hops(t):
        for hop in range(1, last + 1):
            due = t + 1 - LAG * hop
            if 0 <= due < len(jobs):
                pl.when(hops[jobs[due][0]] == hop)(functools.partial(sum_z, *jobs[due]))

    def reduce(k, j):
        for s in range(subs):
            sum_x(k, j, s)
            jobs.append((k, j, s))
            sum_hops(len(jobs) - 1)

    def multiply_partner(j):
        for h in range(2):
            to_p[j, h].wait_recv()
        multiply(1, j)

    def multiply_across(j):
        for h in range(2):
            to_y[j, h].wait_recv()
            fwd[j, h].start()
        multiply(2, j)
        for h in range(2):
            fwd[j, h].wait_recv()
        multiply(3, j)

    for j, h in both:
        own[j, h].wait()
        mk[:, :LANES] = masked(0, j, h)
        for e in range(2):
            lhs_t[e, h * width + j * LANES:h * width + (j + 1) * LANES, :] = mk[e * half:(e + 1) * half, :LANES].T
    for j in range(chunks):
        multiply(0, j)
    multiply_partner(0)
    for j in range(chunks):
        reduce(0, j)
    for j in range(chunks):
        multiply_across(j)
        reduce(1, j)
        if j + 1 < chunks:
            multiply_partner(j + 1)
        reduce(2, j)
        reduce(3, j)
    for t in range(len(jobs), len(jobs) + LAG * last):
        sum_hops(t)

    @pl.when(mirrored)
    def _():
        mine = jnp.where(z == across, 2, 3)
        for first in range(chunks):
            for s in range(first, tiles, chunks):
                for j in range(chunks):
                    part = pl.ds(s * SUB, SUB)
                    remote(zb.at[mine, j, part], mr.at[j, s], msend.at[j, s], mrecv.at[j, s],
                           {"aux": r * 2, "row": z}).wait_recv()
                    out_ref[part, j * LANES:(j + 1) * LANES] = zb[mine, j, part, :] + mr[j, s].T
        for j in range(chunks):
            for s in range(tiles):
                m_copy(mine, j, s).wait_send()

    for w in both:
        to_y[w].wait_send()
        to_p[w].wait_send()
        fwd[w].wait_send()
    for k in range(n_row):
        for j in range(chunks):
            for s in range(subs):
                x_copy(k, j, s).wait_send()
                pl.when(z != owner[k])(lambda: z_copy(k, j, s, True).wait_send())


def solution(mesh):
    n_aux, n_row = mesh.shape["aux"], mesh.shape["row"]

    def local(slabs, significant):
        aux_here, occupied, rows = slabs.shape
        nbf = rows * n_row
        cols = nbf // n_aux
        if n_row != 4 or n_aux != 2 * n_row or cols % LANES or rows % SUB or occupied % 16 or aux_here % 2:
            return plain(slabs, significant)
        chunks = cols // LANES
        depth = aux_here * occupied
        mask = jnp.repeat(significant.astype(jnp.bfloat16), BS, axis=1)
        mask = mask.reshape(aux_here, n_row, 2, chunks, LANES).transpose(1, 2, 3, 0, 4)
        mask = jnp.broadcast_to(mask[:, :, :, :, None], (n_row, 2, chunks, aux_here, 16, LANES))
        dma = pltpu.SemaphoreType.DMA
        subs = rows // SUB
        return pl.pallas_call(
            functools.partial(kernel, n_aux, n_row, occupied),
            out_shape=jax.ShapeDtypeStruct((rows, cols), jnp.float32),
            in_specs=[pl.BlockSpec(memory_space=pl.ANY), pl.BlockSpec(memory_space=pltpu.VMEM)],
            out_specs=pl.BlockSpec(memory_space=pltpu.VMEM),
            scratch_shapes=[
                pltpu.VMEM((2, chunks, 2, depth, LANES), jnp.bfloat16),
                pltpu.VMEM((2, chunks, 2, depth // 2, LANES), jnp.bfloat16),
                pltpu.VMEM((2, rows, depth // 2), jnp.bfloat16),
                pltpu.VMEM((depth, 2 * LANES), jnp.bfloat16),
                pltpu.VMEM((n_row, chunks, 2, rows, LANES), jnp.float32),
            ]
            + [pltpu.VMEM((n_row, chunks, rows, LANES), jnp.float32)] * 4
            + [pltpu.VMEM((chunks, subs, SUB, LANES), jnp.float32)]
            + [dma((chunks, 2))] * 7
            + [dma((n_row, chunks, subs))] * 5
            + [dma((chunks, subs))] * 2,
            compiler_params=pltpu.CompilerParams(
                collective_id=0, has_side_effects=True, vmem_limit_bytes=60 * 2**20
            ),
            cost_estimate=pl.CostEstimate(
                flops=2 * rows * nbf * depth, bytes_accessed=2 * depth * rows, transcendentals=0
            ),
        )(slabs.reshape(depth, rows), mask)

    return jax.shard_map(
        local,
        mesh=mesh,
        in_specs=(P("aux", None, "row"), P("aux", None)),
        out_specs=P("row", "aux"),
        check_vma=False,
    )
```
